64 devices in a mesh: rep: 8 (over x, y, core), dp: 8 (over z).
Axes of the slice: x: 2, y: 2, z: 8, core: 2. Of those that a mesh axis runs over, the one named last changes fastest.
The devices are a block of a 4x4x8 slice.
Arguments:
- x: bfloat16 [64, 2048, 640], P(('rep', 'dp')), parts along dimension 0
- dy: bfloat16 [64, 2048, 640], P(('rep', 'dp')), parts along dimension 0
- w_gate: bfloat16 [2, 640, 2048], replicated
- w_up: bfloat16 [2, 640, 2048], replicated
- w_down: bfloat16 [2, 2048, 640], replicated
- m_w_gate: float32 [2, 640, 2048], P(None, 'dp')
- m_w_up: float32 [2, 640, 2048], P(None, 'dp')
- m_w_down: float32 [2, 2048, 640], P(None, 'dp')
- v_w_gate: float32 [2, 640, 2048], P(None, 'dp')
- v_w_up: float32 [2, 640, 2048], P(None, 'dp')
- v_w_down: float32 [2, 2048, 640], P(None, 'dp')
Outputs:
- output 1: bfloat16 [16, 640, 2048], P('rep'), parts along dimension 0
- output 2: bfloat16 [16, 640, 2048], P('rep'), parts along dimension 0
- output 3: bfloat16 [16, 2048, 640], P('rep'), parts along dimension 0
- output 4: float32 [16, 640, 2048], P('rep', 'dp'), parts along dimension 0
- output 5: float32 [16, 640, 2048], P('rep', 'dp'), parts along dimension 0
- output 6: float32 [16, 2048, 640], P('rep', 'dp'), parts along dimension 0
- output 7: float32 [16, 640, 2048], P('rep', 'dp'), parts along dimension 0
- output 8: float32 [16, 640, 2048], P('rep', 'dp'), parts along dimension 0
- output 9: float32 [16, 2048, 640], P('rep', 'dp'), parts along dimension 0
There are 8 independent parts. The reference program is written for one: setup_inputs(seed, part) draws one part's arguments, and reference() takes and returns one part's arrays. A program takes and returns all parts, laid end to end along the dimension named above; an argument that names none is the same for every part.
All inputs are finite; a program needn't handle non-finite values.
Results may differ from the reference program's by a relative error of at most 0.022.
Values are sent between devices in bfloat16 or wider.
A program may use at most 768 MiB of HBM per device.

```python
import jax
import jax.numpy as jnp
from jax import lax

SEQUENCES = 8
TOKENS = 2048
D = 640
FF = 2048
LAYERS = 2
NAMES = ("w_gate", "w_up", "w_down")
SHAPES = {"w_gate": (LAYERS, D, FF), "w_up": (LAYERS, D, FF), "w_down": (LAYERS, FF, D)}


def bump(key, n, height):
    away = (jnp.arange(n, dtype=jnp.int32) - jax.random.randint(key, (), 0, n, jnp.int32)) % n
    return jnp.where(away < n // 8, height, 1.0)


def together(key, own, strength):
    shared = jax.random.normal(key, own.shape[1:], jnp.float32)
    return (own + strength * shared) * lax.rsqrt(1 + strength * strength)


def setup_inputs(seed: int = 0, part: int = 0) -> dict:
    kx, kdy, ka, kb, kz, kf, kh, kl, *keys = jax.random.split(jax.random.key(seed), 8 + 3 * len(NAMES))
    kx, kdy, ka, kb = (jax.random.fold_in(k, part) for k in (kx, kdy, ka, kb))
    kw, km, kv = (keys[i::3] for i in range(3))
    shape = (SEQUENCES, TOKENS, D)
    much_x, much_dy = jax.random.uniform(kz, (2,), jnp.float32, 0.0, 1.0)
    loud = 2.0 ** jax.random.uniform(jax.random.fold_in(kz, 1), (), jnp.float32, -1.0, 2.0)
    layers = 2.0 ** jax.random.uniform(kl, (LAYERS, 1, 1), jnp.float32, -1.0, 1.0)
    x = together(ka, jax.random.normal(kx, shape, jnp.float32), much_x) * bump(kf, D, 4.0)
    dy = together(kb, jax.random.normal(kdy, shape, jnp.float32), much_dy)
    drawn = {"x": x.astype(jnp.bfloat16), "dy": (loud * dy * (SEQUENCES * TOKENS) ** -0.5).astype(jnp.bfloat16)}
    for key, name in zip(kw, NAMES, strict=True):
        w = jax.random.normal(key, SHAPES[name], jnp.float32) * SHAPES[name][1] ** -0.5
        drawn[name] = (w * {"w_gate": 1.0, "w_up": bump(kh, FF, 4.0), "w_down": layers}[name]).astype(jnp.bfloat16)
    for key, name in zip(km, NAMES, strict=True):
        drawn[f"m_{name}"] = 0.1 * jax.random.normal(key, SHAPES[name], jnp.float32)
    for key, name in zip(kv, NAMES, strict=True):
        drawn[f"v_{name}"] = jax.random.uniform(key, SHAPES[name], jnp.float32, 0.005, 0.015)
    return drawn


def matmul(a, w):
    return jnp.dot(a, w, preferred_element_type=jnp.float32).astype(jnp.bfloat16)


def normed(h):
    wide = h.astype(jnp.float32)
    scale = lax.rsqrt(jnp.mean(wide**2, -1, keepdims=True) + 1e-6)
    return (wide * scale).astype(jnp.bfloat16)


def layer(h, w):
    a = normed(h)
    gate = jnp.dot(a, w["w_gate"], preferred_element_type=jnp.float32)
    up = jnp.dot(a, w["w_up"], preferred_element_type=jnp.float32)
    return h + matmul((jax.nn.silu(gate) * up).astype(jnp.bfloat16), w["w_down"])


def adamw(w, m, v, g):
    m = 0.9 * m + 0.1 * g
    v = 0.95 * v + 0.05 * g * g
    step = m * lax.rsqrt(v + 1e-8) + 0.1 * w
    return (w - 0.02 * step).astype(jnp.bfloat16), m, v


def stack(weights, h):
    return lax.scan(lambda h, w: (layer(h, w), None), h, weights)[0]


def reference(x, dy, w_gate, w_up, w_down, m_w_gate, m_w_up, m_w_down, v_w_gate, v_w_up, v_w_down):
    weights = dict(zip(NAMES, (w_gate, w_up, w_down), strict=True))

    def take(so_far, sequence):
        h, by_y = sequence
        _, back = jax.vjp(lambda w: stack(w, h), weights)
        return jax.tree.map(lambda total, term: total + term.astype(jnp.float32), so_far, back(by_y)[0]), None

    none_yet = {name: jnp.zeros(w.shape, jnp.float32) for name, w in weights.items()}
    by_weights, _ = lax.scan(take, none_yet, (x, dy))
    gradients = [by_weights[name].astype(jnp.bfloat16).astype(jnp.float32) for name in NAMES]
    new = [
        adamw(w.astype(jnp.float32), m, v, g)
        for w, m, v, g in zip((w_gate, w_up, w_down), (m_w_gate, m_w_up, m_w_down), (v_w_gate, v_w_up, v_w_down), gradients, strict=True)
    ]
    return tuple(one[which] for which in range(3) for one in new)
```

```python
import functools

import jax
import jax.numpy as jnp
from jax import lax
from jax.experimental import pallas as pl
from jax.experimental.pallas import tpu as pltpu
from jax.sharding import PartitionSpec as P

MESH = pl.DeviceIdType.MESH
F32, BF16 = jnp.float32, jnp.bfloat16


def dot(a, b, ca, cb):
    return lax.dot_general(a, b, (((ca,), (cb,)), ((), ())), preferred_element_type=F32)


def normed(h):
    wide = h.astype(F32)
    scale = lax.rsqrt(jnp.mean(wide**2, -1, keepdims=True) + 1e-6)
    return (wide * scale).astype(BF16), scale


def norm_back(h, scale, da):
    wide, da = h.astype(F32), da.astype(F32)
    mean = jnp.mean(da * wide, -1, keepdims=True)
    return (da * scale - wide * (scale * scale * scale * mean)).astype(BF16)


def mlp(a, wg, wu):
    return dot(a, wg, 1, 0), dot(a, wu, 1, 0)


def mlp_back(gate, up, dh):
    s = jax.nn.sigmoid(gate)
    silu = gate * s
    dh = dh.astype(F32)
    return (dh * up * (s * (1 + gate * (1 - s)))).astype(BF16), (dh * silu).astype(BF16)


def adamw(w, m, v, g):
    m = 0.9 * m + 0.1 * g
    v = 0.95 * v + 0.05 * g * g
    step = m * lax.rsqrt(v + 1e-8) + 0.1 * w
    return (w - 0.02 * step).astype(BF16), m, v


def gather_kernel(n, layers, *refs):
    ins, outs, (send_sem, recv_sem, own_sem) = refs[:3], refs[3:6], refs[6:]
    me = lax.axis_index("dp")
    right, left = lax.rem(me + 1, n), lax.rem(me + n - 1, n)

    barrier = pltpu.get_barrier_semaphore()
    for neighbour in (left, right):
        pl.semaphore_signal(barrier, inc=1, device_id={"dp": neighbour}, device_id_type=MESH)
    pl.semaphore_wait(barrier, 2)

    items = [(k, layer) for layer in reversed(range(layers)) for k in (2, 0, 1)]

    def half(ref, k, layer, owner, way):
        rows, columns = ins[k].shape[1:]
        if columns % 256 == 0 and k < 2:
            return ref.at[layer, pl.ds(owner * rows, rows), pl.ds(way * (columns // 2), columns // 2)]
        return ref.at[layer, pl.ds(owner * rows + way * (rows // 2), rows // 2), :]

    def copy(i, way, hop):
        k, layer = items[i]
        owner = lax.rem(me + n - hop, n) if way == 0 else lax.rem(me + hop, n)
        src = half(ins[k], k, layer, 0, way) if hop == 0 else half(outs[k], k, layer, owner, way)
        return pltpu.make_async_remote_copy(
            src_ref=src,
            dst_ref=half(outs[k], k, layer, owner, way),
            send_sem=send_sem.at[i, way, hop],
            recv_sem=recv_sem.at[i, way, hop],
            device_id={"dp": right if way == 0 else left},
            device_id_type=MESH,
        )

    mine = []
    for i, (k, layer) in enumerate(items):
        for way in range(2):
            copy(i, way, 0).start()
    for i, (k, layer) in enumerate(items):
        rows = ins[k].shape[1]
        own = pltpu.make_async_copy(ins[k].at[layer], outs[k].at[layer, pl.ds(me * rows, rows), :], own_sem.at[i])
        own.start()
        mine.append(own)
    for hop in range(1, n):
        for i in range(len(items)):
            for way in range(2):
                copy(i, way, hop - 1).wait_recv()
                if hop < n - 1:
                    copy(i, way, hop).start()
    for hop in range(n - 1):
        for i in range(len(items)):
            for way in range(2):
                copy(i, way, hop).wait_send()
    for own in mine:
        own.wait()


def gather(n, blocks):
    layers = blocks[0].shape[0]
    outs = tuple(jax.ShapeDtypeStruct((b.shape[0], b.shape[1] * n, b.shape[2]), b.dtype) for b in blocks)
    vmem = pl.BlockSpec(memory_space=pltpu.VMEM)
    return pl.pallas_call(
        functools.partial(gather_kernel, n, layers),
        out_shape=outs,
        in_specs=[vmem] * 3,
        out_specs=(vmem,) * 3,
        scratch_shapes=[
            pltpu.SemaphoreType.DMA((3 * layers, 2, n - 1)),
            pltpu.SemaphoreType.DMA((3 * layers, 2, n - 1)),
            pltpu.SemaphoreType.DMA((3 * layers,)),
        ],
        compiler_params=pltpu.CompilerParams(collective_id=0, has_side_effects=True, vmem_limit_bytes=40 * 2**20),
    )(*blocks)


def solution(mesh):
    n = mesh.shape["dp"]

    def step(x, dy, *arrays):
        weights, ms, vs = (arrays[i : i + 3] for i in (0, 3, 6))
        x, dy = x[0], dy[0]
        wg, wu, wd = weights
        layers = wg.shape[0]
        saved, h = [], x
        for l in range(layers):
            a, scale = normed(h)
            gate, up = mlp(a, wg[l], wu[l])
            hid = (jax.nn.silu(gate) * up).astype(BF16)
            saved.append((h, a, scale, gate, up, hid))
            if l < layers - 1:
                h = h + dot(hid, wd[l], 1, 0).astype(BF16)
        grads = [[None] * layers for _ in range(3)]

        def reduced(g):
            return lax.psum_scatter(g.astype(BF16), "dp", scatter_dimension=0, tiled=True)

        d = dy
        for l in reversed(range(layers)):
            h, a, scale, gate, up, hid = saved[l]
            grads[2][l] = reduced(dot(hid, d, 0, 0))
            dh = dot(d, wd[l], 1, 1).astype(BF16)
            dgate, dup = mlp_back(gate, up, dh)
            grads[0][l] = reduced(dot(a, dgate, 0, 0))
            grads[1][l] = reduced(dot(a, dup, 0, 0))
            if l:
                da = dot(dgate, wg[l], 1, 1).astype(BF16) + dot(dup, wu[l], 1, 1).astype(BF16)
                d = d + norm_back(h, scale, da)
        me = lax.axis_index("dp")
        new = []
        for w, m, v, g in zip(weights, ms, vs, grads, strict=True):
            g = jnp.stack([t.astype(F32) for t in g])
            own = lax.dynamic_slice_in_dim(w, me * m.shape[1], m.shape[1], 1).astype(F32)
            new.append(adamw(own, m, v, g))
        full = gather(n, [one[0] for one in new])
        return (*full, *(one[1] for one in new), *(one[2] for one in new))

    seq, whole, rows = P(("rep", "dp")), P(), P(None, "dp")
    out_w, out_m = P("rep"), P("rep", "dp")
    return jax.shard_map(
        step,
        mesh=mesh,
        in_specs=(seq, seq, *[whole] * 3, *[rows] * 6),
        out_specs=(*[out_w] * 3, *[out_m] * 6),
        check_vma=False,
    )
```

```python
import functools

import jax
import jax.numpy as jnp
from jax import lax
from jax.experimental import pallas as pl
from jax.experimental.pallas import tpu as pltpu
from jax.sharding import PartitionSpec as P

MESH = pl.DeviceIdType.MESH
F32, BF16 = jnp.float32, jnp.bfloat16
TILE = 256
SLOTS = 4
ANY = pl.BlockSpec(memory_space=pl.ANY)


def dot(a, b, ca, cb):
    return lax.dot_general(a, b, (((ca,), (cb,)), ((), ())), preferred_element_type=F32)


def normed(h):
    wide = h.astype(F32)
    scale = lax.rsqrt(jnp.mean(wide**2, -1, keepdims=True) + 1e-6)
    return (wide * scale).astype(BF16)


def kernel(n, *refs):
    x, dy, wg, wu, wd, mg, mu, md, vg, vu, vd = refs[:11]
    og, ou, od, omg, omu, omd, ovg, ovu, ovd = refs[11:20]
    (a, a_t, d, d_t, h, acc, dgu, hid, wgu, wdn, own_gu, own_d, land, land_d, g_gu, g_d,
     m_gu, v_gu, w_gu, n_gu, m_d, v_d, w_d, n_d,
     rs_send, rs_recv, dn_send, dn_recv, ag_send, ag_recv, own_sem, load_sem, tile_sem, adam_sem, out_sem) = refs[20:]
    tokens, width = h.shape
    tiles = wg.shape[2] // TILE
    chains = 2 * tiles
    rows, rows_d = m_gu.shape[1], m_d.shape[0]
    half = rows_d // 2
    quarter = half // 2
    supers = tiles // 2
    block = tokens // 2
    me = lax.axis_index("dp")
    right, left = lax.rem(me + 1, n), lax.rem(me + n - 1, n)

    barrier = pltpu.get_barrier_semaphore()
    for neighbour in (left, right):
        pl.semaphore_signal(barrier, inc=1, device_id={"dp": neighbour}, device_id_type=MESH)
    def towards(way):
        return {"dp": right if way == 0 else left}

    hops = (n // 2, n - 1 - n // 2)

    def count(part, way):
        return hops[0] if part == way else hops[1]

    def owner_at(step, part, way):
        far = count(part, way) - step
        return lax.rem(me + far, n) if way == 0 else lax.rem(me + n - far, n)

    def place(step, part, way):
        return step if part == way else hops[0] + step

    def ring_copy(ring, c, step, part, way):
        own, land, send_sem, recv_sem = ring
        src = own(c, part, owner_at(0, part, way)) if step == 0 else land.at[c, part, place(step - 1, part, way)]
        here = place(step, part, way)
        return pltpu.make_async_remote_copy(
            src_ref=src, dst_ref=land.at[c, part, here], send_sem=send_sem.at[c, part, way], recv_sem=recv_sem.at[c, part, here],
            device_id=towards(way), device_id_type=MESH,
        )

    def ring_start(ring, c):
        for part in range(2):
            for way in range(2):
                ring_copy(ring, c, 0, part, way).start()

    def ring_step(ring, c, step, finish):
        own, land = ring[:2]
        for part in range(2):
            for way in range(2):
                last = count(part, way)
                if step > last:
                    continue
                ring_copy(ring, c, step - 1, part, way).wait_recv()
                ring_copy(ring, c, step - 1, part, way).wait_send()
                if step < last:
                    at = land.at[c, part, place(step - 1, part, way)]
                    at[...] = (at[...].astype(F32) + own(c, part, owner_at(step, part, way))[...].astype(F32)).astype(BF16)
                    ring_copy(ring, c, step, part, way).start()
        if step == hops[0]:
            for part in range(2):
                total = own(c, part, me)[...].astype(F32)
                for way in range(2):
                    total += land[c, part, place(count(part, way) - 1, part, way)].astype(F32)
                finish(c, part, total.astype(BF16))

    def strips(i):
        t = lax.rem(i, tiles)
        first = lax.rem(t, supers) * 2 * rows_d + (t // supers) * half
        return [pl.ds(pl.multiple_of(first + e * rows_d, half), half) for e in range(2)]

    def tile_loads(i):
        layer, slot = lax.rem(i // tiles, 2), lax.rem(i, 2)
        copies = []
        for e, strip in enumerate(strips(i)):
            here = pl.ds(e * half, half)
            copies += [
                pltpu.make_async_copy(wg.at[layer, :, strip], wgu.at[slot, :, here], tile_sem.at[slot, e, 0]),
                pltpu.make_async_copy(wu.at[layer, :, strip], wgu.at[slot, :, pl.ds(TILE + e * half, half)], tile_sem.at[slot, e, 1]),
                pltpu.make_async_copy(wd.at[layer, strip, :], wdn.at[slot, here, :], tile_sem.at[slot, e, 2]),
            ]
        return copies

    def adam_loads(layer):
        mine = pl.ds(pl.multiple_of(me * rows, 16), rows)
        mine_d = pl.ds(pl.multiple_of(me * rows_d, 16), rows_d)
        pairs = (
            (mg.at[layer], m_gu.at[0]), (mu.at[layer], m_gu.at[1]), (vg.at[layer], v_gu.at[0]), (vu.at[layer], v_gu.at[1]),
            (wg.at[layer, mine, :], w_gu.at[0]), (wu.at[layer, mine, :], w_gu.at[1]),
            (md.at[layer], m_d), (vd.at[layer], v_d), (wd.at[layer, mine_d, :], w_d),
        )
        return [pltpu.make_async_copy(s, t, adam_sem.at[k]) for k, (s, t) in enumerate(pairs)]

    def adam_stores(layer, which):
        gu = ((m_gu.at[0], omg.at[layer]), (m_gu.at[1], omu.at[layer]), (v_gu.at[0], ovg.at[layer]), (v_gu.at[1], ovu.at[layer]))
        down = ((m_d, omd.at[layer]), (v_d, ovd.at[layer]))
        pairs, first = (gu, 0) if which == "gu" else (down, 4)
        return [pltpu.make_async_copy(s, t, out_sem.at[first + k]) for k, (s, t) in enumerate(pairs)]

    def tile_own(c, part, owner):
        return own_gu.at[lax.rem(c, SLOTS), part, pl.ds(pl.multiple_of(owner * rows, 16), rows), :]

    def tile_finish(c, part, total):
        for e, strip in enumerate(strips(c)):
            g_gu[c // tiles, part, :, strip] = total[:, e * half : (e + 1) * half]

    tile_ring = (tile_own, land, rs_send, rs_recv)

    def tile_step(c, step):
        @pl.when((c >= 0) & (c < chains))
        def _():
            ring_step(tile_ring, c, step, tile_finish)

    def down_rows(k, part, owner):
        return pl.ds(pl.multiple_of(owner * rows_d + lax.rem(k, 2) * half + part * quarter, 16), quarter)

    def down_own(k, part, owner):
        return own_d.at[k // 2, down_rows(k, part, owner), :]

    def down_finish(k, part, total):
        g_d[k // 2, down_rows(k, part, 0), :] = total

    down_ring = (down_own, land_d, dn_send, dn_recv)

    def down_steps(i, some):
        for step in some:
            ago = i - supers + 1 - step
            k = ago // supers

            @pl.when((lax.rem(ago, supers) == 0) & (ago >= 0) & (k < 3))
            def _():
                ring_step(down_ring, k, step, down_finish)

    def piece(ref, k, layer, owner, way):
        if k < 2:
            w = ref.shape[-1] // 2
            if layer is None:
                return ref.at[:, pl.ds(way * w, w)]
            return ref.at[layer, pl.ds(pl.multiple_of(owner * rows, 16), rows), pl.ds(way * w, w)]
        if layer is None:
            return ref.at[pl.ds(way * half, half), :]
        return ref.at[layer, pl.ds(pl.multiple_of(owner * rows_d + way * half, 16), half), :]

    def fresh(k, number):
        return (n_gu.at[number, 0], n_gu.at[number, 1], n_d.at[number])[k]

    def ag_copy(number, k, way, hop):
        layer, out = 1 - number, (og, ou, od)[k]
        owner = lax.rem(me + n - hop, n) if way == 0 else lax.rem(me + hop, n)
        dst = piece(out, k, layer, owner, way)
        src = piece(fresh(k, number), k, None, 0, way) if hop == 0 else dst
        item = 3 * number + k
        return pltpu.make_async_remote_copy(
            src_ref=src, dst_ref=dst, send_sem=ag_send.at[item, way], recv_sem=ag_recv.at[item, way, hop],
            device_id=towards(way), device_id_type=MESH,
        )

    def own_copy(number, k):
        layer, out = 1 - number, (og, ou, od)[k]
        count = (rows, rows, rows_d)[k]
        dst = out.at[layer, pl.ds(pl.multiple_of(me * count, 16), count), :]
        return pltpu.make_async_copy(fresh(k, number), dst, own_sem.at[3 * number + k])

    def ag_start(number, k):
        for way in range(2):
            ag_copy(number, k, way, 0).start()
        own_copy(number, k).start()

    def ag_hop(number, k, hop):
        for way in range(2):
            ag_copy(number, k, way, hop - 1).wait_recv()
            ag_copy(number, k, way, hop - 1).wait_send()
            if hop < n - 1:
                ag_copy(number, k, way, hop).start()

    def adamw(w, m, v, g):
        w, g = w[...].astype(F32), g.astype(F32)
        new_m = 0.9 * m[...] + 0.1 * g
        new_v = 0.95 * v[...] + 0.05 * g * g
        m[...] = new_m
        v[...] = new_v
        return (w - 0.02 * (new_m * lax.rsqrt(new_v + 1e-8) + 0.1 * w)).astype(BF16)

    def adam_gu(number):
        for k in range(2):
            n_gu[number, k] = adamw(w_gu.at[k], m_gu.at[k], v_gu.at[k], g_gu[number, k])
        for c in adam_stores(1 - number, "gu"):
            c.start()

    def adam_down(number):
        n_d[number] = adamw(w_d, m_d, v_d, g_d[number])
        for c in adam_stores(1 - number, "down"):
            c.start()

    def turn(src, dst):
        for at in range(0, tokens, TILE):
            dst[:, pl.ds(at, TILE)] = src[pl.ds(at, TILE), :].T

    def forward(i, part):
        slot = lax.rem(i, 2)
        at = pl.ds(part * block, block)
        both = dot(a[at, :], wgu[slot], 1, 0)
        gate, up = both[:, :TILE], both[:, TILE:]
        silu = gate * (0.5 * jnp.tanh(0.5 * gate) + 0.5)
        acc[at, :] += dot((silu * up).astype(BF16), wdn[slot], 1, 0)

    def forward_and_back(i, part, with_da):
        slot = lax.rem(i, 2)
        at = pl.ds(part * block, block)
        both = dot(a[at, :], wgu[slot], 1, 0)
        gate, up = both[:, :TILE], both[:, TILE:]
        dh = dot(d[at, :], wdn[slot], 1, 1).astype(BF16).astype(F32)
        s = 0.5 * jnp.tanh(0.5 * gate) + 0.5
        silu = gate * s
        hid[at, :] = (silu * up).astype(BF16)
        dgu[at, pl.ds(0, TILE)] = (dh * up * (s + silu * (1 - s))).astype(BF16)
        dgu[at, pl.ds(TILE, TILE)] = (dh * silu).astype(BF16)
        if with_da:
            acc[at, :] += dot(dgu[at, :], wgu[slot], 1, 1)

    def weights_back(i):
        both = dot(a_t[...], dgu[...], 1, 0)
        slot = lax.rem(i, SLOTS)
        own_gu[slot, 0] = both[:, :TILE].astype(BF16)
        own_gu[slot, 1] = both[:, TILE:].astype(BF16)

    def down_back(i):
        grad = dot(d_t[...], hid[...], 1, 0).T.astype(BF16)
        for e, strip in enumerate(strips(i)):
            own_d[i // tiles, strip, :] = grad[e * half : (e + 1) * half]

    def steps(i, part):
        for behind, step in (((2, 2),), ((1, 1),), ((3, 4),), ((2, 3),))[part]:
            tile_step(i - behind, step)

    def tile_in(i):
        @pl.when(i + 1 < 3 * tiles)
        def _():
            for c in tile_loads(i + 1):
                c.start()
        for c in tile_loads(i):
            c.wait()

    def one_tile(i, with_da):
        tile_in(i + tiles)
        forward_and_back(i, 0, with_da)
        steps(i, 0)
        forward_and_back(i, 1, with_da)
        steps(i, 1)
        weights_back(i)
        ring_start(tile_ring, i)
        if with_da:
            @pl.when(i == 0)
            def _():
                turn(d, d_t)
        steps(i, 2)
        down_back(i)
        steps(i, 3)
        down_steps(i, range(1, hops[0] + 1))

        @pl.when(lax.rem(i, supers) == supers - 1)
        def _():
            ring_start(down_ring, i // supers)

    def blocks(body):
        @pl.loop(0, tokens // TILE)
        def _(b):
            body(pl.ds(pl.multiple_of(b * TILE, TILE), TILE))

    loads = [pltpu.make_async_copy(s, t, load_sem.at[k]) for k, (s, t) in enumerate(((x, h), (dy, d), (x, a)))]
    loads[0].start()
    for c in tile_loads(0):
        c.start()
    loads[1].start()
    for c in adam_loads(1):
        c.start()
    loads[0].wait()

    def first(at):
        a[at, :] = normed(h[at, :])
        acc[at, :] = jnp.zeros((TILE, width), F32)

    blocks(first)

    @pl.loop(0, tiles)
    def _(i):
        tile_in(i)
        forward(i, 0)
        forward(i, 1)

    def second(at):
        state = (h[at, :].astype(F32) + acc[at, :].astype(BF16).astype(F32)).astype(BF16)
        h[at, :] = state
        a[at, :] = normed(state)
        acc[at, :] = jnp.zeros((TILE, width), F32)

    pl.semaphore_wait(barrier, 2)
    blocks(second)
    turn(a, a_t)
    loads[1].wait()

    @pl.loop(0, tiles)
    def _(i):
        one_tile(i, True)

    loads[2].start()

    def between(at):
        wide = h[at, :].astype(F32)
        da = acc[at, :].astype(BF16).astype(F32)
        scale = lax.rsqrt(jnp.mean(wide * wide, -1, keepdims=True) + 1e-6)
        mean = jnp.mean(da * wide, -1, keepdims=True)
        dn = (da * scale - wide * (scale * scale * scale * mean)).astype(BF16).astype(F32)
        d[at, :] = (d[at, :].astype(F32) + dn).astype(BF16)

    blocks(between)
    turn(d, d_t)
    loads[2].wait()

    def again(at):
        a[at, :] = normed(a[at, :])

    blocks(again)
    turn(a, a_t)

    @pl.loop(tiles, chains)
    def _(i):
        one_tile(i, False)

    for c in adam_loads(1):
        c.wait()
    adam_gu(0)
    adam_down(0)
    for k in range(3):
        ag_start(0, k)

    @pl.loop(chains, chains + 3)
    def _(i):
        for part in range(4):
            steps(i, part)

    for which in ("gu", "down"):
        for c in adam_stores(1, which):
            c.wait()
    for c in adam_loads(0):
        c.start()
    for hop in range(1, n):
        for k in range(3):
            ag_hop(0, k, hop)
        if hop == n - 3:
            for c in adam_loads(0):
                c.wait()
            adam_gu(1)
        if hop == n - 2:
            ag_start(1, 0)
            ag_start(1, 1)
        if hop <= hops[0]:
            ring_step(down_ring, 3, hop, down_finish)
    adam_down(1)
    ag_start(1, 2)
    for hop in range(1, n):
        for k in range(3):
            ag_hop(1, k, hop)
    for which in ("gu", "down"):
        for c in adam_stores(0, which):
            c.wait()
    for number in range(2):
        for k in range(3):
            own_copy(number, k).wait()


def hand_out(*refs):
    ins, outs, held, (in_sem, out_sem) = refs[:9], refs[9:18], refs[18:27], refs[27:]
    pieces = [(k, layer) for layer in range(ins[0].shape[0]) for k in range(9)]
    reads = [pltpu.make_async_copy(ins[k].at[l], held[k].at[l], in_sem.at[k, l]) for k, l in pieces]
    writes = [pltpu.make_async_copy(held[k].at[l], outs[k].at[l], out_sem.at[k, l]) for k, l in pieces]
    for c in reads:
        c.start()
    for r, w in zip(reads, writes, strict=True):
        r.wait()
        w.start()
    for c in writes:
        c.wait()


def solution(mesh):
    n = mesh.shape["dp"]

    def step(x, dy, wg, wu, wd, mg, mu, md, vg, vu, vd):
        x, dy = x[0], dy[0]
        tokens, width = x.shape
        ff = wg.shape[2]
        rows, rows_d = mg.shape[1], md.shape[1]
        tiles = ff // TILE
        shape = jax.ShapeDtypeStruct
        sem, vm = pltpu.SemaphoreType.DMA, pltpu.VMEM
        hop = n - 1
        shapes = tuple(shape(t.shape, t.dtype) for t in (wg, wu, wd, mg, mu, md, vg, vu, vd))
        outs = pl.pallas_call(
            functools.partial(kernel, n),
            out_shape=shapes,
            in_specs=[ANY] * 11,
            out_specs=(ANY,) * 9,
            scratch_shapes=[
                vm((tokens, width), BF16), vm((width, tokens), BF16), vm((tokens, width), BF16), vm((width, tokens), BF16),
                vm((tokens, width), BF16), vm((tokens, width), F32), vm((tokens, 2 * TILE), BF16), vm((tokens, TILE), BF16),
                vm((2, width, 2 * TILE), BF16), vm((2, TILE, width), BF16),
                vm((SLOTS, 2, width, TILE), BF16), vm((2, ff, width), BF16),
                vm((2 * tiles, 2, hop, rows, TILE), BF16), vm((4, 2, hop, rows_d // 4, width), BF16),
                vm((2, 2, rows, ff), BF16), vm((2, rows_d, width), BF16),
                vm((2, rows, ff), F32), vm((2, rows, ff), F32), vm((2, rows, ff), BF16), vm((2, 2, rows, ff), BF16),
                vm((rows_d, width), F32), vm((rows_d, width), F32), vm((rows_d, width), BF16), vm((2, rows_d, width), BF16),
                sem((2 * tiles, 2, 2)), sem((2 * tiles, 2, hop)), sem((4, 2, 2)), sem((4, 2, hop)),
                sem((6, 2)), sem((6, 2, hop)), sem((6,)), sem((3,)), sem((2, 2, 3)), sem((9,)), sem((6,)),
            ],
            compiler_params=pltpu.CompilerParams(collective_id=0, has_side_effects=True, vmem_limit_bytes=67_000_000),
        )(x, dy, wg, wu, wd, mg, mu, md, vg, vu, vd)
        return pl.pallas_call(
            hand_out,
            out_shape=shapes,
            in_specs=[ANY] * 9,
            out_specs=(ANY,) * 9,
            scratch_shapes=[*(vm(t.shape, t.dtype) for t in shapes), sem((9, 2)), sem((9, 2))],
            compiler_params=pltpu.CompilerParams(vmem_limit_bytes=67_000_000),
        )(*outs)

    seq, whole, rows = P(("rep", "dp")), P(), P(None, "dp")
    out_w, out_m = P("rep"), P("rep", "dp")
    return jax.shard_map(
        step,
        mesh=mesh,
        in_specs=(seq, seq, *[whole] * 3, *[rows] * 6),
        out_specs=(*[out_w] * 3, *[out_m] * 6),
        check_vma=False,
    )
```

```python
import functools

import jax
import jax.numpy as jnp
from jax import lax
from jax.experimental import pallas as pl
from jax.experimental.pallas import tpu as pltpu
from jax.sharding import PartitionSpec as P

MESH = pl.DeviceIdType.MESH
F32, BF16 = jnp.float32, jnp.bfloat16
TILE = 256
SLOTS = 4
ANY = pl.BlockSpec(memory_space=pl.ANY)


def dot(a, b, ca, cb):
    return lax.dot_general(a, b, (((ca,), (cb,)), ((), ())), preferred_element_type=F32)


def normed(h):
    wide = h.astype(F32)
    scale = lax.rsqrt(jnp.mean(wide**2, -1, keepdims=True) + 1e-6)
    return (wide * scale).astype(BF16)


def kernel(n, *refs):
    x, dy, wg, wu, wd, mg, mu, md, vg, vu, vd = refs[:11]
    og, ou, od, omg, omu, omd, ovg, ovu, ovd = refs[11:20]
    (a, a_t, d, d_t, h, acc, dgu, hid, wgu, wdn, own_gu, own_d, land, land_d, g_gu, g_d,
     m_gu, v_gu, w_gu, n_gu, m_d, v_d, w_d, n_d,
     rs_send, rs_recv, dn_send, dn_recv, ag_send, ag_recv, own_sem, load_sem, tile_sem, adam_sem, out_sem) = refs[20:]
    tokens, width = h.shape
    tiles = wg.shape[2] // TILE
    chains = 2 * tiles
    rows, rows_d = m_gu.shape[1], m_d.shape[0]
    half = rows_d // 2
    quarter = half // 2
    supers = tiles // 2
    block = tokens // 2
    me = lax.axis_index("dp")
    right, left = lax.rem(me + 1, n), lax.rem(me + n - 1, n)

    barrier = pltpu.get_barrier_semaphore()
    for neighbour in (left, right):
        pl.semaphore_signal(barrier, inc=1, device_id={"dp": neighbour}, device_id_type=MESH)
    def towards(way):
        return {"dp": right if way == 0 else left}

    hops = (n // 2, n - 1 - n // 2)

    def count(part, way):
        return hops[0] if part == way else hops[1]

    def owner_at(step, part, way):
        far = count(part, way) - step
        return lax.rem(me + far, n) if way == 0 else lax.rem(me + n - far, n)

    def place(step, part, way):
        return step if part == way else hops[0] + step

    def ring_copy(ring, c, step, part, way):
        own, land, send_sem, recv_sem = ring
        src = own(c, part, owner_at(0, part, way)) if step == 0 else land.at[c, part, place(step - 1, part, way)]
        here = place(step, part, way)
        return pltpu.make_async_remote_copy(
            src_ref=src, dst_ref=land.at[c, part, here], send_sem=send_sem.at[c, part, way], recv_sem=recv_sem.at[c, part, here],
            device_id=towards(way), device_id_type=MESH,
        )

    def ring_start(ring, c):
        for part in range(2):
            for way in range(2):
                ring_copy(ring, c, 0, part, way).start()

    def ring_step(ring, c, step, finish):
        own, land = ring[:2]
        for part in range(2):
            for way in range(2):
                last = count(part, way)
                if step > last:
                    continue
                ring_copy(ring, c, step - 1, part, way).wait_recv()
                ring_copy(ring, c, step - 1, part, way).wait_send()
                if step < last:
                    at = land.at[c, part, place(step - 1, part, way)]
                    at[...] = (at[...].astype(F32) + own(c, part, owner_at(step, part, way))[...].astype(F32)).astype(BF16)
                    ring_copy(ring, c, step, part, way).start()
        if step == hops[0]:
            for part in range(2):
                total = own(c, part, me)[...].astype(F32)
                for way in range(2):
                    total += land[c, part, place(count(part, way) - 1, part, way)].astype(F32)
                finish(c, part, total.astype(BF16))

    def strips(i):
        t = lax.rem(i, tiles)
        first = lax.rem(t, supers) * 2 * rows_d + (t // supers) * half
        return [pl.ds(pl.multiple_of(first + e * rows_d, half), half) for e in range(2)]

    def tile_loads(i):
        layer, slot = lax.rem(i // tiles, 2), lax.rem(i, 2)
        copies = []
        for e, strip in enumerate(strips(i)):
            here = pl.ds(e * half, half)
            copies += [
                pltpu.make_async_copy(wg.at[layer, :, strip], wgu.at[slot, :, here], tile_sem.at[slot, e, 0]),
                pltpu.make_async_copy(wu.at[layer, :, strip], wgu.at[slot, :, pl.ds(TILE + e * half, half)], tile_sem.at[slot, e, 1]),
                pltpu.make_async_copy(wd.at[layer, strip, :], wdn.at[slot, here, :], tile_sem.at[slot, e, 2]),
            ]
        return copies

    def adam_loads(layer):
        mine = pl.ds(pl.multiple_of(me * rows, 16), rows)
        mine_d = pl.ds(pl.multiple_of(me * rows_d, 16), rows_d)
        pairs = (
            (mg.at[layer], m_gu.at[0]), (mu.at[layer], m_gu.at[1]), (vg.at[layer], v_gu.at[0]), (vu.at[layer], v_gu.at[1]),
            (wg.at[layer, mine, :], w_gu.at[0]), (wu.at[layer, mine, :], w_gu.at[1]),
            (md.at[layer], m_d), (vd.at[layer], v_d), (wd.at[layer, mine_d, :], w_d),
        )
        return [pltpu.make_async_copy(s, t, adam_sem.at[k]) for k, (s, t) in enumerate(pairs)]

    def adam_stores(layer, which):
        gu = ((m_gu.at[0], omg.at[layer]), (m_gu.at[1], omu.at[layer]), (v_gu.at[0], ovg.at[layer]), (v_gu.at[1], ovu.at[layer]))
        down = ((m_d, omd.at[layer]), (v_d, ovd.at[layer]))
        pairs, first = (gu, 0) if which == "gu" else (down, 4)
        return [pltpu.make_async_copy(s, t, out_sem.at[first + k]) for k, (s, t) in enumerate(pairs)]

    def tile_own(c, part, owner):
        return own_gu.at[lax.rem(c, SLOTS), part, pl.ds(pl.multiple_of(owner * rows, 16), rows), :]

    def tile_finish(c, part, total):
        for e, strip in enumerate(strips(c)):
            g_gu[c // tiles, part, :, strip] = total[:, e * half : (e + 1) * half]

    tile_ring = (tile_own, land, rs_send, rs_recv)

    def tile_step(c, step):
        @pl.when((c >= 0) & (c < chains))
        def _():
            ring_step(tile_ring, c, step, tile_finish)

    def down_rows(k, part, owner):
        return pl.ds(pl.multiple_of(owner * rows_d + lax.rem(k, 2) * half + part * quarter, 16), quarter)

    def down_own(k, part, owner):
        return own_d.at[k // 2, down_rows(k, part, owner), :]

    def down_finish(k, part, total):
        g_d[k // 2, down_rows(k, part, 0), :] = total

    down_ring = (down_own, land_d, dn_send, dn_recv)

    def down_steps(i, some):
        for step in some:
            ago = i - supers + 1 - step
            k = ago // supers

            @pl.when((lax.rem(ago, supers) == 0) & (ago >= 0) & (k < 3))
            def _():
                ring_step(down_ring, k, step, down_finish)

    def piece(ref, k, layer, owner, way):
        if k < 2:
            w = ref.shape[-1] // 2
            if layer is None:
                return ref.at[:, pl.ds(way * w, w)]
            return ref.at[layer, pl.ds(pl.multiple_of(owner * rows, 16), rows), pl.ds(way * w, w)]
        if layer is None:
            return ref.at[pl.ds(way * half, half), :]
        return ref.at[layer, pl.ds(pl.multiple_of(owner * rows_d + way * half, 16), half), :]

    def fresh(k, number):
        return (n_gu.at[number, 0], n_gu.at[number, 1], n_d.at[number])[k]

    def ag_copy(number, k, way, hop):
        layer, out = 1 - number, (og, ou, od)[k]
        owner = lax.rem(me + n - hop, n) if way == 0 else lax.rem(me + hop, n)
        dst = piece(out, k, layer, owner, way)
        src = piece(fresh(k, number), k, None, 0, way) if hop == 0 else dst
        item = 3 * number + k
        return pltpu.make_async_remote_copy(
            src_ref=src, dst_ref=dst, send_sem=ag_send.at[item, way], recv_sem=ag_recv.at[item, way, hop],
            device_id=towards(way), device_id_type=MESH,
        )

    def own_copy(number, k):
        layer, out = 1 - number, (og, ou, od)[k]
        count = (rows, rows, rows_d)[k]
        dst = out.at[layer, pl.ds(pl.multiple_of(me * count, 16), count), :]
        return pltpu.make_async_copy(fresh(k, number), dst, own_sem.at[3 * number + k])

    def ag_start(number, k):
        for way in range(2):
            ag_copy(number, k, way, 0).start()
        own_copy(number, k).start()

    def ag_hop(number, k, hop):
        for way in range(2):
            ag_copy(number, k, way, hop - 1).wait_recv()
            ag_copy(number, k, way, hop - 1).wait_send()
            if hop < n - 1:
                ag_copy(number, k, way, hop).start()

    def adamw(w, m, v, g):
        w, g = w[...].astype(F32), g.astype(F32)
        new_m = 0.9 * m[...] + 0.1 * g
        new_v = 0.95 * v[...] + 0.05 * g * g
        m[...] = new_m
        v[...] = new_v
        return (w - 0.02 * (new_m * lax.rsqrt(new_v + 1e-8) + 0.1 * w)).astype(BF16)

    def adam_gu(number):
        for k in range(2):
            n_gu[number, k] = adamw(w_gu.at[k], m_gu.at[k], v_gu.at[k], g_gu[number, k])
        for c in adam_stores(1 - number, "gu"):
            c.start()

    def adam_down(number):
        n_d[number] = adamw(w_d, m_d, v_d, g_d[number])
        for c in adam_stores(1 - number, "down"):
            c.start()

    def turn(src, dst):
        for at in range(0, tokens, TILE):
            dst[:, pl.ds(at, TILE)] = src[pl.ds(at, TILE), :].T

    def forward(i, part):
        slot = lax.rem(i, 2)
        at = pl.ds(part * block, block)
        both = dot(a[at, :], wgu[slot], 1, 0)
        gate, up = both[:, :TILE], both[:, TILE:]
        silu = gate * (0.5 * jnp.tanh(0.5 * gate) + 0.5)
        acc[at, :] += dot((silu * up).astype(BF16), wdn[slot], 1, 0)

    def forward_and_back(i, part, with_da):
        slot = lax.rem(i, 2)
        at = pl.ds(part * block, block)
        both = dot(a[at, :], wgu[slot], 1, 0)
        gate, up = both[:, :TILE], both[:, TILE:]
        dh = dot(d[at, :], wdn[slot], 1, 1).astype(BF16).astype(F32)
        s = 0.5 * jnp.tanh(0.5 * gate) + 0.5
        silu = gate * s
        hid[at, :] = (silu * up).astype(BF16)
        dgu[at, pl.ds(0, TILE)] = (dh * up * (s + silu * (1 - s))).astype(BF16)
        dgu[at, pl.ds(TILE, TILE)] = (dh * silu).astype(BF16)
        if with_da:
            acc[at, :] += dot(dgu[at, :], wgu[slot], 1, 1)

    def weights_back(i):
        both = dot(a_t[...], dgu[...], 1, 0)
        slot = lax.rem(i, SLOTS)
        own_gu[slot, 0] = both[:, :TILE].astype(BF16)
        own_gu[slot, 1] = both[:, TILE:].astype(BF16)

    def down_back(i):
        grad = dot(d_t[...], hid[...], 1, 0).T.astype(BF16)
        for e, strip in enumerate(strips(i)):
            own_d[i // tiles, strip, :] = grad[e * half : (e + 1) * half]

    def steps(i, part):
        for behind, step in (((2, 2),), ((1, 1),), ((3, 4),), ((2, 3),))[part]:
            tile_step(i - behind, step)

    def tile_in(i):
        @pl.when(i + 1 < 3 * tiles)
        def _():
            for c in tile_loads(i + 1):
                c.start()
        for c in tile_loads(i):
            c.wait()

    def one_tile(i, with_da):
        tile_in(i + tiles)
        forward_and_back(i, 0, with_da)
        steps(i, 0)
        forward_and_back(i, 1, with_da)
        steps(i, 1)
        weights_back(i)
        ring_start(tile_ring, i)
        if with_da:
            @pl.when(i == 0)
            def _():
                turn(d, d_t)
        steps(i, 2)
        down_back(i)
        steps(i, 3)
        down_steps(i, range(1, hops[0] + 1))

        @pl.when(lax.rem(i, supers) == supers - 1)
        def _():
            ring_start(down_ring, i // supers)

    def blocks(body):
        @pl.loop(0, tokens // TILE)
        def _(b):
            body(pl.ds(pl.multiple_of(b * TILE, TILE), TILE))

    loads = [pltpu.make_async_copy(s, t, load_sem.at[k]) for k, (s, t) in enumerate(((x, h), (dy, d), (x, a)))]
    loads[0].start()
    for c in tile_loads(0):
        c.start()
    loads[1].start()
    for c in adam_loads(1):
        c.start()
    loads[0].wait()

    def first(at):
        a[at, :] = normed(h[at, :])
        acc[at, :] = jnp.zeros((TILE, width), F32)

    blocks(first)

    @pl.loop(0, tiles)
    def _(i):
        tile_in(i)
        forward(i, 0)
        forward(i, 1)

    def second(at):
        state = (h[at, :].astype(F32) + acc[at, :].astype(BF16).astype(F32)).astype(BF16)
        h[at, :] = state
        a[at, :] = normed(state)
        acc[at, :] = jnp.zeros((TILE, width), F32)

    pl.semaphore_wait(barrier, 2)
    blocks(second)
    turn(a, a_t)
    loads[1].wait()

    @pl.loop(0, tiles)
    def _(i):
        one_tile(i, True)

    loads[2].start()

    def between(at):
        wide = h[at, :].astype(F32)
        da = acc[at, :].astype(BF16).astype(F32)
        scale = lax.rsqrt(jnp.mean(wide * wide, -1, keepdims=True) + 1e-6)
        mean = jnp.mean(da * wide, -1, keepdims=True)
        dn = (da * scale - wide * (scale * scale * scale * mean)).astype(BF16).astype(F32)
        d[at, :] = (d[at, :].astype(F32) + dn).astype(BF16)

    blocks(between)
    turn(d, d_t)
    loads[2].wait()

    def again(at):
        a[at, :] = normed(a[at, :])

    blocks(again)
    turn(a, a_t)

    @pl.loop(tiles, chains)
    def _(i):
        one_tile(i, False)

    for c in adam_loads(1):
        c.wait()
    adam_gu(0)
    adam_down(0)
    for k in range(3):
        ag_start(0, k)

    for hop in range(1, n):
        if hop < hops[0]:
            for part in range(4):
                steps(me * 0 + chains + hop - 1, part)
        if hop == hops[0]:
            for which in ("gu", "down"):
                for c in adam_stores(1, which):
                    c.wait()
            for c in adam_loads(0):
                c.start()
        for k in range(3):
            ag_hop(0, k, hop)
        if hop == n - 3:
            for c in adam_loads(0):
                c.wait()
            adam_gu(1)
        if hop == n - 2:
            ag_start(1, 0)
            ag_start(1, 1)
        if hop <= hops[0]:
            ring_step(down_ring, 3, hop, down_finish)
    adam_down(1)
    ag_start(1, 2)
    for hop in range(1, n):
        for k in range(3):
            ag_hop(1, k, hop)
    for which in ("gu", "down"):
        for c in adam_stores(0, which):
            c.wait()
    for number in range(2):
        for k in range(3):
            own_copy(number, k).wait()


def hand_out(*refs):
    ins, outs, held, (in_sem, out_sem) = refs[:9], refs[9:18], refs[18:27], refs[27:]
    pieces = [(k, layer) for layer in range(ins[0].shape[0]) for k in range(9)]
    reads = [pltpu.make_async_copy(ins[k].at[l], held[k].at[l], in_sem.at[k, l]) for k, l in pieces]
    writes = [pltpu.make_async_copy(held[k].at[l], outs[k].at[l], out_sem.at[k, l]) for k, l in pieces]
    for c in reads:
        c.start()
    for r, w in zip(reads, writes, strict=True):
        r.wait()
        w.start()
    for c in writes:
        c.wait()


def solution(mesh):
    n = mesh.shape["dp"]

    def step(x, dy, wg, wu, wd, mg, mu, md, vg, vu, vd):
        x, dy = x[0], dy[0]
        tokens, width = x.shape
        ff = wg.shape[2]
        rows, rows_d = mg.shape[1], md.shape[1]
        tiles = ff // TILE
        shape = jax.ShapeDtypeStruct
        sem, vm = pltpu.SemaphoreType.DMA, pltpu.VMEM
        hop = n - 1
        shapes = tuple(shape(t.shape, t.dtype) for t in (wg, wu, wd, mg, mu, md, vg, vu, vd))
        outs = pl.pallas_call(
            functools.partial(kernel, n),
            out_shape=shapes,
            in_specs=[ANY] * 11,
            out_specs=(ANY,) * 9,
            scratch_shapes=[
                vm((tokens, width), BF16), vm((width, tokens), BF16), vm((tokens, width), BF16), vm((width, tokens), BF16),
                vm((tokens, width), BF16), vm((tokens, width), F32), vm((tokens, 2 * TILE), BF16), vm((tokens, TILE), BF16),
                vm((2, width, 2 * TILE), BF16), vm((2, TILE, width), BF16),
                vm((SLOTS, 2, width, TILE), BF16), vm((2, ff, width), BF16),
                vm((2 * tiles, 2, hop, rows, TILE), BF16), vm((4, 2, hop, rows_d // 4, width), BF16),
                vm((2, 2, rows, ff), BF16), vm((2, rows_d, width), BF16),
                vm((2, rows, ff), F32), vm((2, rows, ff), F32), vm((2, rows, ff), BF16), vm((2, 2, rows, ff), BF16),
                vm((rows_d, width), F32), vm((rows_d, width), F32), vm((rows_d, width), BF16), vm((2, rows_d, width), BF16),
                sem((2 * tiles, 2, 2)), sem((2 * tiles, 2, hop)), sem((4, 2, 2)), sem((4, 2, hop)),
                sem((6, 2)), sem((6, 2, hop)), sem((6,)), sem((3,)), sem((2, 2, 3)), sem((9,)), sem((6,)),
            ],
            compiler_params=pltpu.CompilerParams(collective_id=0, has_side_effects=True, vmem_limit_bytes=67_000_000),
        )(x, dy, wg, wu, wd, mg, mu, md, vg, vu, vd)
        return pl.pallas_call(
            hand_out,
            out_shape=shapes,
            in_specs=[ANY] * 9,
            out_specs=(ANY,) * 9,
            scratch_shapes=[*(vm(t.shape, t.dtype) for t in shapes), sem((9, 2)), sem((9, 2))],
            compiler_params=pltpu.CompilerParams(vmem_limit_bytes=67_000_000),
        )(*outs)

    seq, whole, rows = P(("rep", "dp")), P(), P(None, "dp")
    out_w, out_m = P("rep"), P("rep", "dp")
    return jax.shard_map(
        step,
        mesh=mesh,
        in_specs=(seq, seq, *[whole] * 3, *[rows] * 6),
        out_specs=(*[out_w] * 3, *[out_m] * 6),
        check_vma=False,
    )
```
